32 devices in a mesh: af: 4 (over z), gx: 2 (over x), gy: 4 (over y, core).
Axes of the slice: x: 2, y: 2, z: 4, core: 2. Of those that a mesh axis runs over, the one named last changes fastest.
Arguments:
- source: float32 [4, 2048, 2048], P('af', ('gx', 'gy')), parts along dimension 0, may hold values from -0.8 to 0.8
- screening: float32 [4], P('af'), parts along dimension 0, may hold values from 0.0002 to 0.002
Outputs:
- solution: float32 [4, 2048, 2048], P('af', ('gx', 'gy')), parts along dimension 0
The draws below stay inside these ranges and needn't reach their ends.
There are 4 independent parts, one for each index of `af`. The reference program is written for one: setup_inputs(seed, part) draws one part's arguments, and reference() takes and returns one part's arrays. A program takes and returns all parts, laid end to end along the dimension named above; each array names one. Nothing has to cross between parts.
All inputs are finite; a program needn't handle non-finite values.
Results may differ from the reference program's by a relative error of at most 0.0014.
Values sent between devices are 32-bit elements; how exact they have to be, the bound alone decides.
A program may use at most 128 MiB of HBM per device.

```python
import math
import jax
import jax.numpy as jnp
from jax import lax

FIELDS = 1
NX = 2048
NY = 2048
N_GX = 2
N_GY = 4


def draw_source(key, part):
    rough_key = jax.random.fold_in(key, 0)
    return jnp.clip(0.1 * jax.random.normal(rough_key, (FIELDS, NX, NY), jnp.float32), -0.6, 0.6)


def setup_inputs(seed: int = 0, part: int = 0) -> dict:
    arg_keys = jax.random.split(jax.random.key(seed), 3)
    part_keys = jax.random.split(jax.random.fold_in(arg_keys[2], part), 3)
    return {
        "source": draw_source(jax.random.fold_in(jax.random.fold_in(arg_keys[2], part), 71), part),
        "screening": jnp.clip(jnp.exp(jax.random.uniform(part_keys[1], (FIELDS,), jnp.float32, math.log(0.0002), math.log(0.002))), 0.0002, 0.002),
    }


HIGHEST = lax.Precision.HIGHEST

def sine_table(length):
    numbers = jnp.arange(length, dtype=jnp.int32) + 1
    phases = numbers[:, None] * numbers[None, :] % (2 * length + 2)
    return math.sqrt(2.0 / (length + 1)) * jnp.sin(phases.astype(jnp.float32) * (math.pi / (length + 1)))

def diagonal_factor(screening, length):
    numbers = (jnp.arange(length, dtype=jnp.int32) + 1).astype(jnp.float32)
    return 4.0 + screening[:, None] - 2.0 * jnp.cos(numbers * (math.pi / (length + 1)))[None, :]

def shift_rows(values, offset, fill_value):
    row_count = values.shape[-2]
    pad_shape = values.shape[:-2] + (abs(offset), values.shape[-1])
    padding = jnp.full(pad_shape, fill_value, values.dtype)
    if offset > 0:
        return jnp.concatenate([padding, values[..., :row_count - offset, :]], axis=-2)
    return jnp.concatenate([values[..., -offset:, :], padding], axis=-2)

def cyclic_solve(low_band, middle, up_band, all_sides):
    row_count = middle.shape[-2]
    stride = 1
    while stride < row_count:
        left_ratio = low_band / shift_rows(middle, stride, 1.0)
        right_ratio = up_band / shift_rows(middle, -stride, 1.0)
        next_low = -left_ratio * shift_rows(low_band, stride, 0.0)
        next_up = -right_ratio * shift_rows(up_band, -stride, 0.0)
        middle = middle - left_ratio * shift_rows(up_band, stride, 0.0) - right_ratio * shift_rows(low_band, -stride, 0.0)
        all_sides = tuple((each_side - left_ratio * shift_rows(each_side, stride, 0.0) - right_ratio * shift_rows(each_side, -stride, 0.0) for each_side in all_sides))
        low_band, up_band = (next_low, next_up)
        stride *= 2
    return tuple((each_side / middle for each_side in all_sides))

def reference(source, screening):
    fields = source.shape[0]
    groups = N_GX * N_GY
    kept_lines = NY // (2 * groups)
    inner_lines = kept_lines - 1
    transform = sine_table(NX)
    spectrum = jnp.einsum('fiy,ki->fyk', source, transform, precision=HIGHEST)
    paired = spectrum.reshape(fields, NY // 2, 2, NX)
    even_lines = paired[:, :, 0, :]
    odd_lines = paired[:, :, 1, :]
    factor = diagonal_factor(screening, NX)[:, None, :]
    later_even = jnp.concatenate([even_lines[:, 1:, :], jnp.zeros_like(even_lines[:, :1, :])], axis=1)
    reduced = (even_lines + factor * odd_lines + later_even).reshape(fields, groups, kept_lines, NX)
    center = (factor * factor - 2.0)[:, None, :, :]
    band_shape = (fields, groups, inner_lines, NX)
    row_index = lax.broadcasted_iota(jnp.int32, band_shape, 2)
    low_band = jnp.where(row_index > 0, -1.0, 0.0)
    up_band = jnp.where(row_index < inner_lines - 1, -1.0, 0.0)
    middle = jnp.broadcast_to(center, band_shape)
    first_unit = jnp.where(row_index == 0, 1.0, 0.0)
    last_unit = jnp.where(row_index == inner_lines - 1, 1.0, 0.0)
    base_part, left_spike, right_spike = cyclic_solve(low_band, middle, up_band, (reduced[:, :, :inner_lines, :], first_unit, last_unit))
    sides_all = reduced[:, :, inner_lines, :] + base_part[:, :, inner_lines - 1, :]
    heads_all = base_part[:, :, 0, :]
    later_heads = jnp.concatenate([heads_all[:, 1:, :], jnp.zeros_like(heads_all[:, :1, :])], axis=1)
    chain_side = sides_all + later_heads
    tail_left = left_spike[:, 0, inner_lines - 1, :][:, None, :]
    head_left = left_spike[:, 0, 0, :][:, None, :]
    head_right = right_spike[:, 0, 0, :][:, None, :]
    tail_right = right_spike[:, 0, inner_lines - 1, :][:, None, :]
    chain_center = center[:, 0]
    chain_index = lax.broadcasted_iota(jnp.int32, (fields, groups, NX), 1)
    last_row = chain_index == groups - 1
    chain_mid = jnp.where(last_row, chain_center + 1.0 - tail_right, chain_center - tail_right - head_left)
    chain_low = jnp.where(chain_index > 0, -tail_left, 0.0)
    chain_up = jnp.where(last_row, 0.0, -head_right)
    separators, = cyclic_solve(chain_low, chain_mid, chain_up, (chain_side,))
    before = jnp.concatenate([jnp.zeros_like(separators[:, :1, :]), separators[:, :-1, :]], axis=1)
    interior = base_part + before[:, :, None, :] * left_spike + separators[:, :, None, :] * right_spike
    kept_values = jnp.concatenate([interior, separators[:, :, None, :]], axis=2).reshape(fields, NY // 2, NX)
    earlier_odd = jnp.concatenate([jnp.zeros_like(kept_values[:, :1, :]), kept_values[:, :-1, :]], axis=1)
    even_values = (even_lines + earlier_odd + kept_values) / factor
    merged = jnp.stack([even_values, kept_values], axis=2).reshape(fields, NY, NX)
    return jnp.einsum('fyk,ki->fiy', merged, transform, precision=HIGHEST)
```

```python
import functools
import math

import jax
import jax.numpy as jnp
import numpy as np
from jax import lax
from jax.experimental import pallas as pl
from jax.experimental.pallas import tpu as pltpu
from jax.sharding import PartitionSpec as P

LANES = 128
SEGMENTS = 8
TILE = 256
STEP = 32
GRID_AXES = ("gx", "gy")


def mode_numbers(length):
    half = length // 2
    numbers = np.arange(half, dtype=np.int64) + 1
    return np.concatenate([2 * numbers, length + 1 - 2 * numbers])


def double_cosines(length):
    angles = mode_numbers(length).astype(np.float32) * np.float32(math.pi / (length + 1))
    return (np.float32(2.0) * np.cos(angles.astype(np.float64)).astype(np.float32))[None, :]


def angle_tables(length):
    half = length // 2
    columns = np.arange(half, dtype=np.int64)[None, :] + 1
    coarse = np.arange(half // STEP, dtype=np.int64)[:, None] * STEP
    fine = np.arange(STEP, dtype=np.int64)[:, None] + 1
    scale = math.sqrt(2.0 / (length + 1))
    angle = lambda rows: 2.0 * math.pi * (rows * columns % (length + 1)) / (length + 1)
    tables = (
        scale * np.sin(angle(coarse)),
        scale * np.cos(angle(coarse)),
        np.sin(angle(fine)),
        np.cos(angle(fine)),
    )
    return tuple(table.astype(np.float32) for table in tables)


def power(base, exponent):
    result = None
    while exponent:
        if exponent & 1:
            result = base if result is None else result * base
        exponent >>= 1
        if exponent:
            base = base * base
    return result


def decay_of(screening, cosines):
    factor = (4.0 + screening) - cosines
    excess = factor - 2.0
    root = jnp.sqrt(excess * (excess + 4.0))
    return 2.0 / (factor + root), root


def split(values):
    high = values.astype(jnp.bfloat16)
    return high, (values - high.astype(jnp.float32)).astype(jnp.bfloat16)


def mirrored(values):
    lanes = lax.broadcasted_iota(jnp.int32, values.shape, 1)
    return jnp.take_along_axis(values, LANES - 1 - lanes, axis=1)


def parity(shape):
    lanes = lax.broadcasted_iota(jnp.int32, shape, 1)
    return jnp.where(lanes % 2 == 0, 1.0, -1.0)


def table_tile(tables, table_high, table_low, columns):
    coarse_sin, coarse_cos, fine_sin, fine_cos = tables
    for a in range(coarse_sin.shape[0]):
        values = (
            coarse_sin[a : a + 1, columns] * fine_cos[:, columns]
            + coarse_cos[a : a + 1, columns] * fine_sin[:, columns]
        )
        high, low = split(values)
        table_high[a * STEP : (a + 1) * STEP, columns] = high
        table_low[a * STEP : (a + 1) * STEP, columns] = low


def product(high, low, table_high, table_low, columns):
    dot = functools.partial(jnp.dot, preferred_element_type=jnp.float32)
    return (
        dot(high[...], table_high[:, columns])
        + dot(low[...], table_high[:, columns])
        + dot(high[...], table_low[:, columns])
    )


def forward_kernel(
    source, screening, cosines, coarse_sin, coarse_cos, fine_sin, fine_cos,
    spectrum, left_parts, right_parts, moments,
    high, low, table_high, table_low, stage, arrived,
):
    tables = (coarse_sin, coarse_cos, fine_sin, fine_cos)
    rows, length = source.shape
    blocks = length // LANES
    copies = [
        pltpu.make_async_copy(source.at[:, pl.ds(c * LANES, LANES)], stage.at[c], arrived.at[c])
        for c in range(blocks)
    ]
    for copy in copies:
        copy.start()
    half = length // 2
    steps = rows // SEGMENTS
    signs = parity((2 * SEGMENTS, LANES))
    for copy in copies:
        copy.wait()
    for c in range(blocks // 2):
        columns = pl.ds(c * LANES, LANES)
        for g in range(0, steps, 2):
            place = pl.ds(g * SEGMENTS, 2 * SEGMENTS)
            place_sum = pl.ds(rows + g * SEGMENTS, 2 * SEGMENTS)

            def load(column):
                pair = [stage[column, pl.ds(g + e, SEGMENTS, stride=steps), :] for e in range(2)]
                return jnp.concatenate(pair, axis=0)

            near = load(c)
            far = mirrored(load(blocks - 1 - c))
            high[place, columns], low[place, columns] = split(near - far)
            high[place_sum, columns], low[place_sum, columns] = split((near + far) * signs)
    for t in range(half // TILE):
        columns = pl.ds(t * TILE, TILE)
        table_tile(tables, table_high, table_low, columns)
        values = product(high, low, table_high, table_low, columns)
        spectrum[:, t * TILE : (t + 1) * TILE] = values[:rows]
        spectrum[:, half + t * TILE : half + (t + 1) * TILE] = values[rows:]
    decay, _ = decay_of(screening[0], cosines[...])
    stride = power(decay, steps)
    for t in range(length // TILE):
        columns = slice(t * TILE, (t + 1) * TILE)
        ratio = jnp.broadcast_to(decay[:, columns], (SEGMENTS, TILE))
        left = right = jnp.zeros((SEGMENTS, TILE), jnp.float32)
        for g in range(steps):
            mirror = steps - 1 - g
            left = ratio * left + spectrum[g * SEGMENTS : (g + 1) * SEGMENTS, columns]
            right = ratio * right + spectrum[mirror * SEGMENTS : (mirror + 1) * SEGMENTS, columns]
        left_parts[:, columns] = left
        right_parts[:, columns] = right
    left = right = jnp.zeros((1, length), jnp.float32)
    for s in range(SEGMENTS):
        left = stride * left + left_parts[s : s + 1, :]
        right = stride * right + right_parts[SEGMENTS - 1 - s : SEGMENTS - s, :]
    moments[0:1, :] = left
    moments[1:2, :] = right


def backward_kernel(
    groups, spectrum, left_parts, right_parts, all_moments, screening, cosines,
    coarse_sin, coarse_cos, fine_sin, fine_cos,
    solved, high, low, table_high, table_low, left_states, right_states, stage, stored,
):
    tables = (coarse_sin, coarse_cos, fine_sin, fine_cos)
    rows, length = spectrum.shape
    half = length // 2
    steps = rows // SEGMENTS
    position = lax.axis_index(GRID_AXES)
    decay, root = decay_of(screening[0], cosines[...])
    stride = power(decay, steps)
    block = power(decay, rows)
    whole = power(decay, rows * groups + 1)
    left_total = right_total = jnp.zeros((1, length), jnp.float32)
    for d in range(groups):
        left_total = block * left_total + all_moments[2 * d : 2 * d + 1, :]
        e = groups - 1 - d
        right_total = block * right_total + all_moments[2 * e + 1 : 2 * e + 2, :]
    edge = -decay / (1.0 - whole * whole)
    left_state = edge * (right_total - whole * left_total)
    right_state = edge * (left_total - whole * right_total)
    left_own, right_own = left_state, right_state
    for d in range(groups):
        left_own = jnp.where(d == position, left_state, left_own)
        left_state = block * left_state + all_moments[2 * d : 2 * d + 1, :]
        e = groups - 1 - d
        right_own = jnp.where(e == position, right_state, right_own)
        right_state = block * right_state + all_moments[2 * e + 1 : 2 * e + 2, :]
    after_states = []
    for s in range(SEGMENTS):
        left_states[s : s + 1, :] = left_own
        left_own = stride * left_own + left_parts[s : s + 1, :]
        after_states.append(left_own)
    for s in reversed(range(SEGMENTS)):
        right_states[s : s + 1, :] = (right_own + decay * after_states[s]) / root
        right_own = stride * right_own + right_parts[s : s + 1, :]
    for t in range(length // TILE):
        columns = slice(t * TILE, (t + 1) * TILE)
        ratio = jnp.broadcast_to(decay[:, columns], (SEGMENTS, TILE))
        state = left_states[:, columns]
        sums = []
        for g in range(steps):
            state = ratio * state + spectrum[g * SEGMENTS : (g + 1) * SEGMENTS, columns]
            sums.append(state)
        state = right_states[:, columns]
        first = rows * (t * TILE // half)
        inner = slice(t * TILE % half, t * TILE % half + TILE)
        for g in reversed(range(0, steps, 2)):
            later = ratio * (state + sums[g + 1])
            state = ratio * (later + sums[g])
            place = pl.ds(first + g * SEGMENTS, 2 * SEGMENTS)
            high[place, inner], low[place, inner] = split(jnp.concatenate([state, later], axis=0))
    signs = parity((SEGMENTS, LANES))
    blocks = length // LANES
    copies = []
    for t in range(half // TILE):
        table_tile(tables, table_high, table_low, pl.ds(t * TILE, TILE))
        values = product(high, low, table_high, table_low, pl.ds(t * TILE, TILE))
        for c in range(TILE // LANES):
            near = t * TILE // LANES + c
            far = blocks - 1 - near
            columns = slice(c * LANES, (c + 1) * LANES)
            for g in range(steps):
                place = pl.ds(g, SEGMENTS, stride=steps)
                odd = values[g * SEGMENTS : (g + 1) * SEGMENTS, columns]
                even = values[rows + g * SEGMENTS : rows + (g + 1) * SEGMENTS, columns] * signs
                stage[near, place, :] = even + odd
                stage[far, place, :] = mirrored(even - odd)
            for block_index in (near, far):
                target = solved.at[:, pl.ds(block_index * LANES, LANES)]
                copy = pltpu.make_async_copy(stage.at[block_index], target, stored.at[block_index])
                copy.start()
                copies.append(copy)
    for copy in copies:
        copy.wait()


def on_device(source, screening):
    groups = lax.axis_size(GRID_AXES)
    fields, rows, length = source.shape
    half = length // 2
    tables = [jnp.asarray(table) for table in angle_tables(length)]
    cosines = jnp.asarray(double_cosines(length))
    vmem = pl.BlockSpec(memory_space=pltpu.VMEM)
    smem = pl.BlockSpec(memory_space=pltpu.SMEM)
    f32 = lambda *shape: jax.ShapeDtypeStruct(shape, jnp.float32)
    scratch = [
        pltpu.VMEM((2 * rows, half), jnp.bfloat16),
        pltpu.VMEM((2 * rows, half), jnp.bfloat16),
        pltpu.VMEM((half, half), jnp.bfloat16),
        pltpu.VMEM((half, half), jnp.bfloat16),
    ]
    staging = [
        pltpu.VMEM((length // LANES, rows, LANES), jnp.float32),
        pltpu.SemaphoreType.DMA((length // LANES,)),
    ]
    hbm = pl.BlockSpec(memory_space=pl.ANY)
    parts = (SEGMENTS, length)
    params = pltpu.CompilerParams(vmem_limit_bytes=40 * 2**20)

    def one_field(grid, constant):
        spectrum, left_parts, right_parts, moments = pl.pallas_call(
            forward_kernel,
            out_shape=[f32(rows, length), f32(*parts), f32(*parts), f32(2, length)],
            in_specs=[hbm, smem] + [vmem] * 5,
            out_specs=[vmem] * 4,
            scratch_shapes=scratch + staging,
            compiler_params=params,
            name="forward",
        )(grid, constant, cosines, *tables)
        all_moments = lax.all_gather(moments, GRID_AXES, axis=0, tiled=True)
        return pl.pallas_call(
            functools.partial(backward_kernel, groups),
            out_shape=f32(rows, length),
            in_specs=[vmem] * 4 + [smem] + [vmem] * 5,
            out_specs=hbm,
            scratch_shapes=scratch + [pltpu.VMEM(parts, jnp.float32)] * 2 + staging,
            compiler_params=params,
            name="backward",
        )(spectrum, left_parts, right_parts, all_moments, constant, cosines, *tables)

    return jnp.stack([one_field(source[f], screening[f : f + 1]) for f in range(fields)])


def solution(mesh):
    return jax.shard_map(
        on_device,
        mesh=mesh,
        in_specs=(P("af", GRID_AXES, None), P("af")),
        out_specs=P("af", GRID_AXES, None),
        check_vma=False,
    )
```

```python
import functools
import math

import jax
import jax.numpy as jnp
import numpy as np
from jax import lax
from jax.experimental import pallas as pl
from jax.experimental.pallas import tpu as pltpu
from jax.sharding import PartitionSpec as P

LANES = 128
SEGMENTS = 8
TILE = 256
STEP = 32
GRID_AXES = ("gx", "gy")
MESH = pl.DeviceIdType.MESH


def mode_numbers(length):
    half = length // 2
    numbers = np.arange(half, dtype=np.int64) + 1
    return np.concatenate([2 * numbers, length + 1 - 2 * numbers])


def double_cosines(length):
    angles = mode_numbers(length).astype(np.float32) * np.float32(math.pi / (length + 1))
    return (np.float32(2.0) * np.cos(angles.astype(np.float64)).astype(np.float32))[None, :]


def angle_tables(length):
    half = length // 2
    columns = np.arange(half, dtype=np.int64)[None, :] + 1
    coarse = np.arange(half // STEP, dtype=np.int64)[:, None] * STEP
    fine = np.arange(STEP, dtype=np.int64)[:, None] + 1
    scale = math.sqrt(2.0 / (length + 1))
    angle = lambda rows: 2.0 * math.pi * (rows * columns % (length + 1)) / (length + 1)
    tables = (
        scale * np.sin(angle(coarse)),
        scale * np.cos(angle(coarse)),
        np.sin(angle(fine)),
        np.cos(angle(fine)),
    )
    return tuple(table.astype(np.float32) for table in tables)


def power(base, exponent):
    result = None
    while exponent:
        if exponent & 1:
            result = base if result is None else result * base
        exponent >>= 1
        if exponent:
            base = base * base
    return result


def decay_of(screening, cosines):
    factor = (4.0 + screening) - cosines
    excess = factor - 2.0
    root = jnp.sqrt(excess * (excess + 4.0))
    return 2.0 / (factor + root), root


def split(values):
    high = values.astype(jnp.bfloat16)
    return high, (values - high.astype(jnp.float32)).astype(jnp.bfloat16)


def mirrored(values):
    lanes = lax.broadcasted_iota(jnp.int32, values.shape, 1)
    return jnp.take_along_axis(values, LANES - 1 - lanes, axis=1)


def parity(shape):
    lanes = lax.broadcasted_iota(jnp.int32, shape, 1)
    return jnp.where(lanes % 2 == 0, 1.0, -1.0)


def table_tile(tables, table_high, table_low, columns):
    coarse_sin, coarse_cos, fine_sin, fine_cos = tables
    for a in range(coarse_sin.shape[0]):
        values = (
            coarse_sin[a : a + 1, columns] * fine_cos[:, columns]
            + coarse_cos[a : a + 1, columns] * fine_sin[:, columns]
        )
        high, low = split(values)
        table_high[a * STEP : (a + 1) * STEP, columns] = high
        table_low[a * STEP : (a + 1) * STEP, columns] = low


def product(high, low, table_high, table_low, columns):
    dot = functools.partial(jnp.dot, preferred_element_type=jnp.float32)
    return (
        dot(high[...], table_high[:, columns])
        + dot(low[...], table_high[:, columns])
        + dot(high[...], table_low[:, columns])
    )


def peer(index):
    across = lax.axis_size("gy")
    return {"gx": index // across, "gy": index % across}


def forward_kernel(
    groups, source, screening, cosines, coarse_sin, coarse_cos, fine_sin, fine_cos,
    spectrum, left_parts, right_parts, all_moments,
    high, low, table_high, table_low, stage, arrived,
    moments, landed, send_sems, recv_sems,
):
    tables = (coarse_sin, coarse_cos, fine_sin, fine_cos)
    rows, length = source.shape
    blocks = length // LANES
    copies = [
        pltpu.make_async_copy(source.at[:, pl.ds(c * LANES, LANES)], stage.at[c], arrived.at[c])
        for c in range(blocks)
    ]
    for copy in copies:
        copy.start()
    half = length // 2
    steps = rows // SEGMENTS
    position = lax.axis_index(GRID_AXES)
    barrier = pltpu.get_barrier_semaphore()
    for d in range(1, groups):
        pl.semaphore_signal(barrier, inc=1, device_id=peer((position + d) % groups), device_id_type=MESH)
    signs = parity((2 * SEGMENTS, LANES))
    for copy in copies:
        copy.wait()
    for c in range(blocks // 2):
        columns = pl.ds(c * LANES, LANES)
        for g in range(0, steps, 2):
            place = pl.ds(g * SEGMENTS, 2 * SEGMENTS)
            place_sum = pl.ds(rows + g * SEGMENTS, 2 * SEGMENTS)

            def load(column):
                pair = [stage[column, pl.ds(g + e, SEGMENTS, stride=steps), :] for e in range(2)]
                return jnp.concatenate(pair, axis=0)

            near = load(c)
            far = mirrored(load(blocks - 1 - c))
            high[place, columns], low[place, columns] = split(near - far)
            high[place_sum, columns], low[place_sum, columns] = split((near + far) * signs)
    for t in range(half // TILE):
        columns = pl.ds(t * TILE, TILE)
        table_tile(tables, table_high, table_low, columns)
        values = product(high, low, table_high, table_low, columns)
        spectrum[:, t * TILE : (t + 1) * TILE] = values[:rows]
        spectrum[:, half + t * TILE : half + (t + 1) * TILE] = values[rows:]
    decay, _ = decay_of(screening[0], cosines[...])
    stride = power(decay, steps)
    for t in range(length // TILE):
        columns = slice(t * TILE, (t + 1) * TILE)
        ratio = jnp.broadcast_to(decay[:, columns], (SEGMENTS, TILE))
        left = right = jnp.zeros((SEGMENTS, TILE), jnp.float32)
        for g in range(steps):
            mirror = steps - 1 - g
            left = ratio * left + spectrum[g * SEGMENTS : (g + 1) * SEGMENTS, columns]
            right = ratio * right + spectrum[mirror * SEGMENTS : (mirror + 1) * SEGMENTS, columns]
        left_parts[:, columns] = left
        right_parts[:, columns] = right
    left = right = jnp.zeros((1, length), jnp.float32)
    for s in range(SEGMENTS):
        left = stride * left + left_parts[s : s + 1, :]
        right = stride * right + right_parts[SEGMENTS - 1 - s : SEGMENTS - s, :]
    moments[0:1, :] = left
    moments[1:2, :] = right
    pl.semaphore_wait(barrier, groups - 1)
    sends = []
    for d in range(1, groups):
        send = pltpu.make_async_remote_copy(
            src_ref=moments,
            dst_ref=landed.at[position],
            send_sem=send_sems.at[d],
            recv_sem=recv_sems.at[position],
            device_id=peer((position + d) % groups),
            device_id_type=MESH,
        )
        send.start()
        sends.append(send)
    all_moments[position] = moments[...]
    for d in range(1, groups):
        origin = (position + groups - d) % groups
        pltpu.make_async_remote_copy(
            src_ref=moments,
            dst_ref=landed.at[origin],
            send_sem=send_sems.at[d],
            recv_sem=recv_sems.at[origin],
            device_id=peer(origin),
            device_id_type=MESH,
        ).wait_recv()
        all_moments[origin] = landed[origin]
    for send in sends:
        send.wait_send()


def backward_kernel(
    groups, spectrum, left_parts, right_parts, all_moments, screening, cosines,
    coarse_sin, coarse_cos, fine_sin, fine_cos,
    solved, high, low, table_high, table_low, left_states, right_states, stage, stored,
):
    tables = (coarse_sin, coarse_cos, fine_sin, fine_cos)
    rows, length = spectrum.shape
    half = length // 2
    steps = rows // SEGMENTS
    position = lax.axis_index(GRID_AXES)
    decay, root = decay_of(screening[0], cosines[...])
    stride = power(decay, steps)
    block = power(decay, rows)
    whole = power(decay, rows * groups + 1)
    left_total = right_total = jnp.zeros((1, length), jnp.float32)
    for d in range(groups):
        left_total = block * left_total + all_moments[d, 0:1, :]
        e = groups - 1 - d
        right_total = block * right_total + all_moments[e, 1:2, :]
    edge = -decay / (1.0 - whole * whole)
    left_state = edge * (right_total - whole * left_total)
    right_state = edge * (left_total - whole * right_total)
    left_own, right_own = left_state, right_state
    for d in range(groups):
        left_own = jnp.where(d == position, left_state, left_own)
        left_state = block * left_state + all_moments[d, 0:1, :]
        e = groups - 1 - d
        right_own = jnp.where(e == position, right_state, right_own)
        right_state = block * right_state + all_moments[e, 1:2, :]
    after_states = []
    for s in range(SEGMENTS):
        left_states[s : s + 1, :] = left_own
        left_own = stride * left_own + left_parts[s : s + 1, :]
        after_states.append(left_own)
    for s in reversed(range(SEGMENTS)):
        right_states[s : s + 1, :] = (right_own + decay * after_states[s]) / root
        right_own = stride * right_own + right_parts[s : s + 1, :]
    for t in range(length // TILE):
        columns = slice(t * TILE, (t + 1) * TILE)
        ratio = jnp.broadcast_to(decay[:, columns], (SEGMENTS, TILE))
        state = left_states[:, columns]
        sums = []
        for g in range(steps):
            state = ratio * state + spectrum[g * SEGMENTS : (g + 1) * SEGMENTS, columns]
            sums.append(state)
        state = right_states[:, columns]
        first = rows * (t * TILE // half)
        inner = slice(t * TILE % half, t * TILE % half + TILE)
        for g in reversed(range(0, steps, 2)):
            later = ratio * (state + sums[g + 1])
            state = ratio * (later + sums[g])
            place = pl.ds(first + g * SEGMENTS, 2 * SEGMENTS)
            high[place, inner], low[place, inner] = split(jnp.concatenate([state, later], axis=0))
    signs = parity((SEGMENTS, LANES))
    blocks = length // LANES
    copies = []
    for t in range(half // TILE):
        table_tile(tables, table_high, table_low, pl.ds(t * TILE, TILE))
        values = product(high, low, table_high, table_low, pl.ds(t * TILE, TILE))
        for c in range(TILE // LANES):
            near = t * TILE // LANES + c
            far = blocks - 1 - near
            columns = slice(c * LANES, (c + 1) * LANES)
            for g in range(steps):
                place = pl.ds(g, SEGMENTS, stride=steps)
                odd = values[g * SEGMENTS : (g + 1) * SEGMENTS, columns]
                even = values[rows + g * SEGMENTS : rows + (g + 1) * SEGMENTS, columns] * signs
                stage[near, place, :] = even + odd
                stage[far, place, :] = mirrored(even - odd)
            for block_index in (near, far):
                target = solved.at[:, pl.ds(block_index * LANES, LANES)]
                copy = pltpu.make_async_copy(stage.at[block_index], target, stored.at[block_index])
                copy.start()
                copies.append(copy)
    for copy in copies:
        copy.wait()


def on_device(source, screening):
    groups = lax.axis_size(GRID_AXES)
    fields, rows, length = source.shape
    half = length // 2
    tables = [jnp.asarray(table) for table in angle_tables(length)]
    cosines = jnp.asarray(double_cosines(length))
    vmem = pl.BlockSpec(memory_space=pltpu.VMEM)
    smem = pl.BlockSpec(memory_space=pltpu.SMEM)
    f32 = lambda *shape: jax.ShapeDtypeStruct(shape, jnp.float32)
    scratch = [
        pltpu.VMEM((2 * rows, half), jnp.bfloat16),
        pltpu.VMEM((2 * rows, half), jnp.bfloat16),
        pltpu.VMEM((half, half), jnp.bfloat16),
        pltpu.VMEM((half, half), jnp.bfloat16),
    ]
    staging = [
        pltpu.VMEM((length // LANES, rows, LANES), jnp.float32),
        pltpu.SemaphoreType.DMA((length // LANES,)),
    ]
    hbm = pl.BlockSpec(memory_space=pl.ANY)
    exchange = [
        pltpu.VMEM((2, length), jnp.float32),
        pltpu.VMEM((groups, 2, length), jnp.float32),
        pltpu.SemaphoreType.DMA((groups,)),
        pltpu.SemaphoreType.DMA((groups,)),
    ]
    parts = (SEGMENTS, length)
    params = pltpu.CompilerParams(vmem_limit_bytes=40 * 2**20)

    def one_field(grid, constant):
        spectrum, left_parts, right_parts, all_moments = pl.pallas_call(
            functools.partial(forward_kernel, groups),
            out_shape=[f32(rows, length), f32(*parts), f32(*parts), f32(groups, 2, length)],
            in_specs=[hbm, smem] + [vmem] * 5,
            out_specs=[vmem] * 4,
            scratch_shapes=scratch + staging + exchange,
            compiler_params=pltpu.CompilerParams(
                vmem_limit_bytes=40 * 2**20, collective_id=0, has_side_effects=True
            ),
            name="forward",
        )(grid, constant, cosines, *tables)
        return pl.pallas_call(
            functools.partial(backward_kernel, groups),
            out_shape=f32(rows, length),
            in_specs=[vmem] * 4 + [smem] + [vmem] * 5,
            out_specs=hbm,
            scratch_shapes=scratch + [pltpu.VMEM(parts, jnp.float32)] * 2 + staging,
            compiler_params=params,
            name="backward",
        )(spectrum, left_parts, right_parts, all_moments, constant, cosines, *tables)

    return jnp.stack([one_field(source[f], screening[f : f + 1]) for f in range(fields)])


def solution(mesh):
    return jax.shard_map(
        on_device,
        mesh=mesh,
        in_specs=(P("af", GRID_AXES, None), P("af")),
        out_specs=P("af", GRID_AXES, None),
        check_vma=False,
    )
```
